1024 devices in a mesh: dp: 64 (over x_lo, z, core), tensor: 16 (over y, x_hi).
Axes of the slice: x: 8 (x_hi: 2, x_lo: 4; x = x_hi * 4 + x_lo), y: 8, z: 8, core: 2. Of those that a mesh axis runs over, the one named last changes fastest.
Arguments:
- queries: bfloat16 [28672, 8192], P('dp', 'tensor'), may hold values from -6 to 6
- features: bfloat16 [128, 384, 8192], P('dp', None, 'tensor'), may hold values from -6 to 6
- kv_weight: bfloat16 [8192, 2048], P('tensor'), may hold values from -0.0625 to 0.0625
- q_gain: float32 [128], replicated, may hold values from 0.5 to 2
- k_gain: float32 [128], replicated, may hold values from 0.5 to 2
- counts: int32 [128], replicated, may hold values from 1 to 16, as said below
- owner: int32 [128], replicated, may hold values from 0 to 127, as said below
Outputs:
- attended: bfloat16 [28672, 8192], P('dp', 'tensor')
The draws below stay inside these ranges and needn't reach their ends.
Inputs may be any that keep to these rules, and one draw needn't show every extreme that they name: `counts`: every sample has 1 to 16 images; in every draw some sample has 16 and some has one. `owner`: there are 2 different shifts c_j, each from 0 to the number of dp indices minus 1; sample s = e * 2 + j goes to slot ((e + c_j) modulo the number of dp indices) * 2 + j, with the same c_j for every e.
All inputs are finite; a program needn't handle non-finite values.
Results may differ from the reference program's by a relative error of at most 0.028.
Values may be sent and summed in bfloat16 or wider, within the bound.
A program may use at most 64 MiB of HBM per device.

```python
import math
import jax
import jax.numpy as jnp
from jax import lax

VIS = 8192
QH = 64
KVH = 8
HD = 128
TXT = 224
PATCH = 24
MAX_IMAGES = 16
SAMP_DEV = 2
SAMPLES = 128
N_TENSOR = 16


def draw_counts(key, part):
    first_key, second_key = jax.random.split(jax.random.fold_in(key, 11), 2)
    drawn = jax.random.randint(first_key, (SAMPLES,), 1, MAX_IMAGES + 1).astype(jnp.int32)
    chosen = jax.random.permutation(second_key, SAMPLES)[:2]
    drawn = drawn.at[chosen[0]].set(MAX_IMAGES)
    drawn = drawn.at[chosen[1]].set(1)
    return drawn.astype(jnp.int32)


def draw_owner(key, part):
    shard_total = SAMPLES // SAMP_DEV
    base_key = jax.random.fold_in(key, 23)
    shift_list = jax.random.permutation(base_key, shard_total).astype(jnp.int32)[:SAMP_DEV]
    encoder = jnp.arange(shard_total, dtype=jnp.int32)[:, None]
    position = jnp.arange(SAMP_DEV, dtype=jnp.int32)[None, :]
    target = (encoder + shift_list[None, :]) % shard_total
    return (target * SAMP_DEV + position).reshape(-1).astype(jnp.int32)


def shard_levels(own_key, extent, cuts, low, largest):
    factor_of = 1.0
    for dim, blocks in cuts:
        draws = jax.random.uniform(jax.random.fold_in(jax.random.fold_in(own_key, 6), dim), (blocks,), jnp.float32, low / len(cuts), largest / len(cuts))
        factor_of = factor_of * jnp.repeat(jnp.exp(draws), extent[dim] // blocks).reshape((-1,) + (1,) * (len(extent) - 1 - dim))
    return factor_of


def scatter_about(own_key, dims, deviation, most, shards=(), kind=jnp.bfloat16):
    result = deviation * jax.random.normal(own_key, dims, jnp.float32)
    if shards:
        result = result * shard_levels(own_key, dims, shards, -0.22, 0.18)
    return jnp.clip(result, -most, most).astype(kind)


def setup_inputs(seed: int = 0) -> dict:
    arg_keys = jax.random.split(jax.random.key(seed), 8)
    queries = scatter_about(arg_keys[0], (SAMPLES * TXT, QH * HD), 1.0, 6.0, ((0, 64), (1, 16)))
    features = scatter_about(arg_keys[1], (SAMPLES, MAX_IMAGES * PATCH, VIS), 1.0, 6.0, ((0, 64), (2, 16)))
    kv_weight = scatter_about(arg_keys[2], (VIS, 2 * KVH * HD), VIS ** -0.5, 0.0625, ((0, 16),))
    q_gain = jnp.clip(jnp.exp(jax.random.uniform(arg_keys[3], (HD,), jnp.float32, math.log(0.5), math.log(2.0))), 0.5, 2.0)
    k_gain = jnp.clip(jnp.exp(jax.random.uniform(arg_keys[4], (HD,), jnp.float32, math.log(0.5), math.log(2.0))), 0.5, 2.0)
    counts = draw_counts(jax.random.fold_in(arg_keys[7], 71), 0)
    owner = draw_owner(jax.random.fold_in(arg_keys[7], 71), 0)
    return {"queries": queries, "features": features, "kv_weight": kv_weight, "q_gain": q_gain, "k_gain": k_gain, "counts": counts, "owner": owner}


def normalize_rows(values_in, gain):
    return values_in * lax.rsqrt(lax.optimization_barrier(jnp.mean(values_in * values_in, axis=-1, keepdims=True)) + 1e-05) * gain

def reference(queries, features, kv_weight, q_gain, k_gain, counts, owner):
    group_size = QH // KVH
    token_count = features.shape[1]
    piece_width = VIS // N_TENSOR
    weight_groups = kv_weight.astype(jnp.float32).reshape(N_TENSOR, piece_width, 2 * KVH * HD)
    source_of = jnp.zeros((SAMPLES,), jnp.int32).at[owner].set(jnp.arange(SAMPLES, dtype=jnp.int32))
    query_blocks = queries.reshape(SAMPLES, TXT, QH, HD)

    def attend_slot(slot_id):
        sample = source_of[slot_id]
        feature_rows = features[sample].astype(jnp.float32).reshape(token_count, N_TENSOR, piece_width)
        partials = jnp.einsum('rnc,ncf->nrf', feature_rows, weight_groups)
        partials = lax.optimization_barrier(partials.astype(jnp.bfloat16)).astype(jnp.float32)
        projected = lax.optimization_barrier(jnp.sum(partials, axis=0)).reshape(token_count, KVH, 2, HD)
        key_heads = normalize_rows(projected[:, :, 0], k_gain).astype(jnp.bfloat16)
        value_heads = projected[:, :, 1].astype(jnp.bfloat16)
        query_here = normalize_rows(query_blocks[slot_id].astype(jnp.float32), q_gain) / math.sqrt(HD)
        query_here = lax.optimization_barrier(query_here.astype(jnp.bfloat16)).astype(jnp.float32)
        key_here = jnp.repeat(key_heads, group_size, axis=1).astype(jnp.float32)
        value_here = jnp.repeat(value_heads, group_size, axis=1).astype(jnp.float32)
        scores = jnp.einsum('tqd,rqd->qtr', query_here, key_here)
        valid_keys = jnp.arange(token_count, dtype=jnp.int32) < counts[sample] * PATCH
        exponent = jnp.where(valid_keys[None, None, :], jnp.exp(scores), 0.0)
        weights = (exponent / lax.optimization_barrier(jnp.sum(exponent, axis=-1, keepdims=True))).astype(jnp.bfloat16)
        weights = lax.optimization_barrier(weights).astype(jnp.float32)
        context = jnp.einsum('qtr,rqd->tqd', weights, value_here)
        return context.astype(jnp.bfloat16).reshape(TXT, QH * HD)
    attended = lax.map(attend_slot, jnp.arange(SAMPLES, dtype=jnp.int32))
    return attended.reshape(SAMPLES * TXT, QH * HD)
```

```python
import functools
import math

import jax
import jax.numpy as jnp
from jax import lax
from jax.experimental import pallas as pl
from jax.experimental.pallas import tpu as pltpu
from jax.sharding import Mesh
from jax.sharding import PartitionSpec as P

KVH = 8
HD = 128
PATCH = 24
PIECES = 8
COPIES = 18
DP = ("x_lo", "z", "core")
TENSOR = ("y", "x_hi")
MESH = pl.DeviceIdType.MESH


def wrap(value, size):
    return lax.rem(value + 2 * size, size)


def exchange(
    pieces, owner_ref, feat_ref, weight_ref, gain_ref, out_ref,
    partner, chosen, first, left0, right0, left1, right1, left, right,
    summed, cross, ready, near, turned, far, spun, side, twin_k, twin_v,
    send_sem, recv_sem, core_send, core_recv,
):
    x_lo, z, core = lax.axis_index("x_lo"), lax.axis_index("z"), lax.axis_index("core")
    y, x_hi = lax.axis_index("y"), lax.axis_index("x_hi")
    x = x_hi * 4 + x_lo
    samples = feat_ref.shape[0]
    tokens = feat_ref.shape[1]
    rows = samples * tokens // pieces
    per_sample = pieces // samples

    def at_x(by):
        there = wrap(x + by, 8)
        return {"x_lo": lax.rem(there, 4), "x_hi": there // 4}

    def at_y(by):
        return {"y": wrap(y + by, 8)}

    def at_z(by):
        return {"z": wrap(z + by, 8)}

    other_core = {"core": 1 - core}

    barrier = pltpu.get_barrier_semaphore()
    peers = [at_y(-1), at_y(1), at_x(-2), at_x(2), at_x(-1), at_x(1)]
    peers += [at_z(-1), at_z(1), at_z(-3), at_z(3), other_core]
    for peer in peers:
        pl.semaphore_signal(barrier, inc=1, device_id=peer, device_id_type=MESH)
    pl.semaphore_wait(barrier, len(peers))

    core_copies = []
    for j in range(samples):
        copy = pltpu.make_async_remote_copy(
            src_ref=feat_ref.at[j], dst_ref=partner.at[j],
            send_sem=core_send.at[j], recv_sem=core_recv.at[j],
            device_id=other_core, device_id_type=MESH,
        )
        copy.start()
        core_copies.append(copy)

    place = z * 2 + core
    plan = []
    for j in range(samples):
        shift = owner_ref[j] // samples
        swap = lax.rem(shift, 2)
        low = lax.rem(shift, 16)
        borrow = jnp.where(place < low, 1, 0)
        along_z = lax.rem(lax.rem(shift // 2, 8) + swap * (1 - core), 8)
        along_x = lax.rem(shift // 16 + borrow + 2, 4)
        plan.append((swap, along_z, along_x))

    copies = {}

    def send(piece, number, source, target, device):
        copy = pltpu.make_async_remote_copy(
            src_ref=source, dst_ref=target,
            send_sem=send_sem.at[piece * COPIES + number],
            recv_sem=recv_sem.at[piece * COPIES + number],
            device_id=device, device_id_type=MESH,
        )
        copy.start()
        copies[piece, number] = copy

    def arrive(piece, *numbers):
        for number in numbers:
            copies[piece, number].wait_recv()

    def partial(piece, by):
        head = wrap(y + by, 8)
        columns = pl.ds(pl.multiple_of(head * 2 * HD, 2 * HD), 2 * HD)
        return jnp.dot(
            chosen[pl.ds(piece * rows, rows), :], weight_ref[:, columns],
            preferred_element_type=jnp.float32,
        )

    def widen(value):
        return value.astype(jnp.float32)

    def narrow(value):
        return value.astype(jnp.bfloat16)

    def start_piece(p):
        j = p // per_sample
        if p % per_sample == 0:
            core_copies[j].wait_recv()
            swapped = jnp.full((tokens, 1), plan[j][0], jnp.int32) == 1
            chosen[pl.ds(j * tokens, tokens), :] = jnp.where(swapped, partner[j], feat_ref[j])
        first[p] = narrow(partial(p, 4))
        send(p, 0, first.at[p, :, pl.ds(0, HD)], left0.at[p], at_y(-1))
        send(p, 1, first.at[p, :, pl.ds(HD, HD)], right0.at[p], at_y(1))

    def second(p):
        to_left, to_right = partial(p, -3), partial(p, 3)
        arrive(p, 0, 1)
        left1[p, :, pl.ds(0, HD)] = narrow(to_left[:, :HD] + widen(left0[p]))
        left1[p, :, pl.ds(HD, HD)] = narrow(to_left[:, HD:])
        send(p, 2, left1.at[p], left.at[p, 0], at_y(-1))
        right1[p, :, pl.ds(0, HD)] = narrow(to_right[:, :HD])
        right1[p, :, pl.ds(HD, HD)] = narrow(to_right[:, HD:] + widen(right0[p]))
        send(p, 3, right1.at[p], right.at[p, 0], at_y(1))

    def later(p, step):
        to_left, to_right = partial(p, step - 3), partial(p, 3 - step)
        arrive(p, 2 * step, 2 * step + 1)
        left[p, step - 1] = narrow(to_left + widen(left[p, step - 1]))
        send(p, 2 * step + 2, left.at[p, step - 1], left.at[p, step], at_y(-1))
        right[p, step - 1] = narrow(to_right + widen(right[p, step - 1]))
        send(p, 2 * step + 3, right.at[p, step - 1], right.at[p, step], at_y(1))

    def own(p):
        mine = partial(p, 0)
        arrive(p, 6, 7)
        summed[p] = narrow(mine + widen(left[p, 2]) + widen(right[p, 2]))
        send(p, 8, summed.at[p], cross.at[p, 0], at_x(2))
        send(p, 9, summed.at[p], cross.at[p, 1], at_x(-2))

    def normed(p):
        arrive(p, 8, 9)
        total = widen(cross[p, 0]) + widen(cross[p, 1])
        keys = total[:, :HD]
        scale = lax.rsqrt(jnp.mean(keys * keys, axis=-1, keepdims=True) + 1e-05)
        ready[p, :, pl.ds(0, HD)] = narrow(keys * scale * gain_ref[...])
        ready[p, :, pl.ds(HD, HD)] = narrow(total[:, HD:])
        send(p, 10, ready.at[p], near.at[p, 0], at_z(1))
        send(p, 11, ready.at[p], near.at[p, 1], at_z(-1))

    def pick(index, options):
        mask = jnp.full((rows, 1), index, jnp.int32)
        result = options[0]
        for number in range(1, len(options)):
            result = jnp.where(mask == number, options[number], result)
        return result

    def turn_near(p):
        arrive(p, 10, 11)
        s = plan[p // per_sample][1]
        plus = (s == 1) | (s == 4) | (s == 6)
        minus = (s == 2) | (s == 7)
        index = jnp.where(plus, 1, jnp.where(minus, 2, 0))
        turned[p] = pick(index, [ready[p], near[p, 0], near[p, 1]])
        send(p, 12, turned.at[p], far.at[p, 0], at_z(3))
        send(p, 13, turned.at[p], far.at[p, 1], at_z(-3))

    def turn_far(p):
        arrive(p, 12, 13)
        s = plan[p // per_sample][1]
        plus = (s == 2) | (s == 3) | (s == 4)
        minus = (s == 5) | (s == 6)
        index = jnp.where(plus, 1, jnp.where(minus, 2, 0))
        spun[p] = pick(index, [turned[p], far[p, 0], far[p, 1]])
        send(p, 14, spun.at[p], side.at[p, 0], at_x(1))
        send(p, 15, spun.at[p], side.at[p, 1], at_x(-1))
        send(p, 16, spun.at[p, :, pl.ds(0, HD)], twin_k.at[p], at_x(2))
        send(p, 17, spun.at[p, :, pl.ds(HD, HD)], twin_v.at[p], at_x(-2))

    def finish(p):
        arrive(p, 14, 15, 16, 17)
        u = plan[p // per_sample][2]
        for half, twin in enumerate((twin_k, twin_v)):
            part = pl.ds(half * HD, HD)
            out_ref[pl.ds(p * rows, rows), part] = pick(
                u, [spun[p, :, part], side[p, 0, :, part], twin[p], side[p, 1, :, part]]
            )

    stages = [start_piece, second, lambda p: later(p, 1), lambda p: later(p, 2), own, normed]
    stages += [turn_near, turn_far, finish]
    for t in range(pieces + len(stages) - 1):
        for number in reversed(range(len(stages))):
            if 0 <= t - number < pieces:
                stages[number](t - number)
    for copy in core_copies:
        copy.wait_send()
    for copy in copies.values():
        copy.wait_send()


def keys_and_values(features, kv_weight, k_gain, owner):
    samples, tokens, width = features.shape
    total = samples * tokens
    rows = total // PIECES
    wide, half = (rows, 2 * HD), (rows, HD)

    def buffers(*shape):
        return pltpu.VMEM((PIECES, *shape), jnp.bfloat16)

    vmem = pl.BlockSpec(memory_space=pltpu.VMEM)
    return pl.pallas_call(
        functools.partial(exchange, PIECES),
        out_shape=jax.ShapeDtypeStruct((total, 2 * HD), jnp.bfloat16),
        in_specs=[pl.BlockSpec(memory_space=pltpu.SMEM), vmem, vmem, vmem],
        out_specs=vmem,
        scratch_shapes=[
            pltpu.VMEM((samples, tokens, width), jnp.bfloat16),
            pltpu.VMEM((total, width), jnp.bfloat16),
            buffers(*wide), buffers(*half), buffers(*half), buffers(*wide), buffers(*wide),
            buffers(3, *wide), buffers(3, *wide),
            buffers(*wide), buffers(2, *wide), buffers(*wide), buffers(2, *wide),
            buffers(*wide), buffers(2, *wide), buffers(*wide), buffers(2, *wide),
            buffers(*half), buffers(*half),
            pltpu.SemaphoreType.DMA((PIECES * COPIES,)),
            pltpu.SemaphoreType.DMA((PIECES * COPIES,)),
            pltpu.SemaphoreType.DMA((samples,)),
            pltpu.SemaphoreType.DMA((samples,)),
        ],
        compiler_params=pltpu.CompilerParams(
            collective_id=0, has_side_effects=True, vmem_limit_bytes=48 * 1024 * 1024
        ),
        name="exchange",
    )(owner, features, kv_weight, k_gain.reshape(1, HD))


def normalize(values_in, gain):
    scale = lax.rsqrt(jnp.mean(values_in * values_in, axis=-1, keepdims=True) + 1e-05)
    return values_in * scale * gain


def shards(queries, features, kv_weight, q_gain, k_gain, counts, owner):
    samples, tokens = features.shape[:2]
    both = keys_and_values(features, kv_weight, k_gain, owner)
    both = both.reshape(samples, tokens, 2 * HD)
    key_heads, value_heads = both[..., :HD], both[..., HD:]
    shifts = owner[:samples] // samples
    shard_count = lax.axis_size(DP)
    source = (lax.axis_index(DP) - shifts) % shard_count * samples
    source = source + jnp.arange(samples, dtype=jnp.int32)
    matches = jnp.arange(counts.shape[0], dtype=jnp.int32)[None, :] == source[:, None]
    slot_count = jnp.sum(jnp.where(matches, counts[None, :], 0), axis=1)
    query_rows = queries.shape[0]
    heads = queries.shape[1] // HD
    text_len = query_rows // samples
    query_float = queries.astype(jnp.float32).reshape(samples, text_len, heads, HD)
    query_normed = (normalize(query_float, q_gain) / math.sqrt(HD)).astype(jnp.bfloat16)
    scores = jnp.einsum(
        "stad,srd->satr", query_normed, key_heads, preferred_element_type=jnp.float32
    )
    valid_keys = jnp.arange(tokens, dtype=jnp.int32)[None, :] < (slot_count * PATCH)[:, None]
    exponent = jnp.where(valid_keys[:, None, None, :], jnp.exp(scores), 0.0)
    weights = (exponent / jnp.sum(exponent, axis=-1, keepdims=True)).astype(jnp.bfloat16)
    context = jnp.einsum(
        "satr,srd->stad", weights, value_heads, preferred_element_type=jnp.float32
    )
    return context.astype(jnp.bfloat16).reshape(query_rows, heads * HD)


def solution(mesh):
    torus = Mesh(mesh.devices.reshape(4, 8, 2, 8, 2), (*DP, *TENSOR))
    in_specs = (P(DP, TENSOR), P(DP, None, TENSOR), P(TENSOR, None), P(), P(), P(), P())
    return jax.shard_map(
        shards, mesh=torus, in_specs=in_specs, out_specs=P(DP, TENSOR), check_vma=False
    )
```

```python
import math

import jax
import jax.numpy as jnp
from jax import lax
from jax.experimental import pallas as pl
from jax.experimental.pallas import tpu as pltpu
from jax.sharding import Mesh
from jax.sharding import PartitionSpec as P

HD = 128
PATCH = 24
PIECES = 12
COPIES = 18
OFFSETS = (0.0, 4.0, 5.5, 7.0, 8.5, 10.0, 11.5, 15.0, 18.0)
QUERY_TIME = 3.9
DP = ("x_lo", "z", "core")
TENSOR = ("y", "x_hi")
MESH = pl.DeviceIdType.MESH


def wrap(value, size):
    return lax.rem(value + 2 * size, size)


def widen(value):
    return value.astype(jnp.float32)


def narrow(value):
    return value.astype(jnp.bfloat16)


def normalize(values_in, gain):
    scale = lax.rsqrt(jnp.mean(values_in * values_in, axis=-1, keepdims=True) + 1e-05)
    return values_in * scale * gain


def body(
    owner_ref, counts_ref, query_hbm, feat_hbm, weight_hbm, q_gain_ref, k_gain_ref, out_hbm,
    query, feat, weight, result, both,
    partner, chosen, first, left0, right0, left1, right1, left, right,
    summed, cross, ready, near, turned, far, spun, side, twin_k, twin_v,
    send_sem, recv_sem, core_send, core_recv, load_sem, store_sem,
):
    x_lo, z, core = lax.axis_index("x_lo"), lax.axis_index("z"), lax.axis_index("core")
    y, x_hi = lax.axis_index("y"), lax.axis_index("x_hi")
    x = x_hi * 4 + x_lo
    samples, tokens = feat_hbm.shape[:2]
    rows = samples * tokens // PIECES
    per_sample = PIECES // samples
    text_len = query_hbm.shape[0] // samples
    heads = query_hbm.shape[1] // HD

    loads = []

    def load(source, target):
        copy = pltpu.make_async_copy(source, target, load_sem.at[len(loads)])
        copy.start()
        loads.append(copy)
        return copy

    feat_loads = [load(feat_hbm.at[j], feat.at[j]) for j in range(samples)]
    weight_load = load(weight_hbm, weight)
    query_load = load(query_hbm, query)

    def at_x(by):
        there = wrap(x + by, 8)
        return {"x_lo": lax.rem(there, 4), "x_hi": there // 4}

    def at_y(by):
        return {"y": wrap(y + by, 8)}

    def at_z(by):
        return {"z": wrap(z + by, 8)}

    other_core = {"core": 1 - core}

    barrier = pltpu.get_barrier_semaphore()
    peers = [at_y(-1), at_y(1), at_x(-2), at_x(2), at_x(-1), at_x(1)]
    peers += [at_z(-1), at_z(1), at_z(-3), at_z(3), other_core]
    for peer in peers:
        pl.semaphore_signal(barrier, inc=1, device_id=peer, device_id_type=MESH)
    pl.semaphore_wait(barrier, len(peers))

    core_copies = []
    for j in range(samples):
        copy = pltpu.make_async_remote_copy(
            src_ref=feat_hbm.at[j], dst_ref=partner.at[j],
            send_sem=core_send.at[j], recv_sem=core_recv.at[j],
            device_id=other_core, device_id_type=MESH,
        )
        copy.start()
        core_copies.append(copy)

    place = z * 2 + core
    plan, valid = [], []
    for j in range(samples):
        shift = owner_ref[j] // samples
        swap = lax.rem(shift, 2)
        low = lax.rem(shift, 16)
        borrow = jnp.where(place < low, 1, 0)
        along_z = lax.rem(lax.rem(shift // 2, 8) + swap * (1 - core), 8)
        along_x = lax.rem(shift // 16 + borrow + 2, 4)
        plan.append((swap, along_z, along_x))
        source = lax.rem(x_lo * 16 + place - shift + 64, 64)
        valid.append(counts_ref[source * samples + j] * PATCH)

    copies = {}

    def send(piece, number, source, target, device):
        copy = pltpu.make_async_remote_copy(
            src_ref=source, dst_ref=target,
            send_sem=send_sem.at[piece * COPIES + number],
            recv_sem=recv_sem.at[piece * COPIES + number],
            device_id=device, device_id_type=MESH,
        )
        copy.start()
        copies[piece, number] = copy

    def arrive(piece, *numbers):
        for number in numbers:
            copies[piece, number].wait_recv()

    def partial(piece, by):
        head = wrap(y + by, 8)
        columns = pl.ds(pl.multiple_of(head * 2 * HD, 2 * HD), 2 * HD)
        return jnp.dot(
            chosen[pl.ds(piece * rows, rows), :], weight[:, columns],
            preferred_element_type=jnp.float32,
        )

    def start_piece(p):
        j = p // per_sample
        if p % per_sample == 0:
            feat_loads[j].wait()
            if j == 0:
                weight_load.wait()
            core_copies[j].wait_recv()
            swapped = jnp.full((tokens, 1), plan[j][0], jnp.int32) == 1
            chosen[pl.ds(j * tokens, tokens), :] = jnp.where(swapped, partner[j], feat[j])
        first[p] = narrow(partial(p, 4))
        send(p, 0, first.at[p, :, pl.ds(0, HD)], left0.at[p], at_y(-1))
        send(p, 1, first.at[p, :, pl.ds(HD, HD)], right0.at[p], at_y(1))

    def second(p):
        to_left, to_right = partial(p, -3), partial(p, 3)
        arrive(p, 0, 1)
        left1[p, :, pl.ds(0, HD)] = narrow(to_left[:, :HD] + widen(left0[p]))
        left1[p, :, pl.ds(HD, HD)] = narrow(to_left[:, HD:])
        send(p, 2, left1.at[p], left.at[p, 0], at_y(-1))
        right1[p, :, pl.ds(0, HD)] = narrow(to_right[:, :HD])
        right1[p, :, pl.ds(HD, HD)] = narrow(to_right[:, HD:] + widen(right0[p]))
        send(p, 3, right1.at[p], right.at[p, 0], at_y(1))

    def later(p, step):
        to_left, to_right = partial(p, step - 3), partial(p, 3 - step)
        arrive(p, 2 * step, 2 * step + 1)
        left[p, step - 1] = narrow(to_left + widen(left[p, step - 1]))
        send(p, 2 * step + 2, left.at[p, step - 1], left.at[p, step], at_y(-1))
        right[p, step - 1] = narrow(to_right + widen(right[p, step - 1]))
        send(p, 2 * step + 3, right.at[p, step - 1], right.at[p, step], at_y(1))

    def own(p):
        mine = partial(p, 0)
        arrive(p, 6, 7)
        summed[p] = narrow(mine + widen(left[p, 2]) + widen(right[p, 2]))
        send(p, 8, summed.at[p], cross.at[p, 0], at_x(2))
        send(p, 9, summed.at[p], cross.at[p, 1], at_x(-2))

    def normed(p):
        arrive(p, 8, 9)
        total = widen(cross[p, 0]) + widen(cross[p, 1])
        ready[p, :, pl.ds(0, HD)] = narrow(normalize(total[:, :HD], k_gain_ref[...]))
        ready[p, :, pl.ds(HD, HD)] = narrow(total[:, HD:])
        send(p, 10, ready.at[p], near.at[p, 0], at_z(1))
        send(p, 11, ready.at[p], near.at[p, 1], at_z(-1))

    def pick(index, options):
        mask = jnp.full((rows, 1), index, jnp.int32)
        chosen_one = options[0]
        for number in range(1, len(options)):
            chosen_one = jnp.where(mask == number, options[number], chosen_one)
        return chosen_one

    def turn_near(p):
        arrive(p, 10, 11)
        s = plan[p // per_sample][1]
        plus = (s == 1) | (s == 4) | (s == 6)
        minus = (s == 2) | (s == 7)
        index = jnp.where(plus, 1, jnp.where(minus, 2, 0))
        turned[p] = pick(index, [ready[p], near[p, 0], near[p, 1]])
        send(p, 12, turned.at[p], far.at[p, 0], at_z(3))
        send(p, 13, turned.at[p], far.at[p, 1], at_z(-3))

    def turn_far(p):
        arrive(p, 12, 13)
        s = plan[p // per_sample][1]
        plus = (s == 2) | (s == 3) | (s == 4)
        minus = (s == 5) | (s == 6)
        index = jnp.where(plus, 1, jnp.where(minus, 2, 0))
        spun[p] = pick(index, [turned[p], far[p, 0], far[p, 1]])
        send(p, 14, spun.at[p], side.at[p, 0], at_x(1))
        send(p, 15, spun.at[p], side.at[p, 1], at_x(-1))
        send(p, 16, spun.at[p, :, pl.ds(0, HD)], twin_k.at[p], at_x(2))
        send(p, 17, spun.at[p, :, pl.ds(HD, HD)], twin_v.at[p], at_x(-2))

    def finish(p):
        arrive(p, 14, 15, 16, 17)
        u = plan[p // per_sample][2]
        for half, twin in enumerate((twin_k, twin_v)):
            part = pl.ds(half * HD, HD)
            both[pl.ds(p * rows, rows), part] = pick(
                u, [spun[p, :, part], side[p, 0, :, part], twin[p], side[p, 1, :, part]]
            )

    def prepare_queries():
        query_load.wait()
        for a in range(heads):
            part = pl.ds(a * HD, HD)
            normed_query = normalize(widen(query[:, part]), q_gain_ref[...])
            query[:, part] = narrow(normed_query / math.sqrt(HD))

    stores = []

    def attend(j):
        held = pl.ds(j * tokens, tokens)
        text = pl.ds(j * text_len, text_len)
        keys, values = both[held, pl.ds(0, HD)], both[held, pl.ds(HD, HD)]
        column = lax.broadcasted_iota(jnp.int32, (text_len, tokens), 1)
        for a in range(heads):
            part = pl.ds(a * HD, HD)
            scores = lax.dot_general(
                query[text, part], keys, (((1,), (1,)), ((), ())),
                preferred_element_type=jnp.float32,
            )
            exponent = jnp.where(column < valid[j], jnp.exp(scores), 0.0)
            weights = narrow(exponent / jnp.sum(exponent, axis=-1, keepdims=True))
            context = jnp.dot(weights, values, preferred_element_type=jnp.float32)
            result[text, part] = narrow(context)
        copy = pltpu.make_async_copy(result.at[text], out_hbm.at[text], store_sem.at[j])
        copy.start()
        stores.append(copy)

    stages = [start_piece, second, lambda p: later(p, 1), lambda p: later(p, 2), own, normed]
    stages += [turn_near, turn_far, finish]
    tasks = [(QUERY_TIME, 1, prepare_queries, ())]
    for number, (stage, offset) in enumerate(zip(stages, OFFSETS)):
        tasks += [(p + offset, -number, stage, (p,)) for p in range(PIECES)]
    for j in range(samples):
        tasks.append(((j + 1) * per_sample - 1 + OFFSETS[-1], 1, attend, (j,)))
    for _, _, task, given in sorted(tasks, key=lambda task: task[:2]):
        task(*given)
    for copy in core_copies + list(copies.values()):
        copy.wait_send()
    for copy in stores:
        copy.wait()


def shards(queries, features, kv_weight, q_gain, k_gain, counts, owner):
    samples, tokens, width = features.shape
    total = samples * tokens
    rows = total // PIECES
    wide, half = (rows, 2 * HD), (rows, HD)

    def whole(*shape):
        return pltpu.VMEM(shape, jnp.bfloat16)

    def buffers(*shape):
        return whole(PIECES, *shape)

    smem = pl.BlockSpec(memory_space=pltpu.SMEM)
    vmem = pl.BlockSpec(memory_space=pltpu.VMEM)
    hbm = pl.BlockSpec(memory_space=pltpu.HBM)
    return pl.pallas_call(
        body,
        out_shape=jax.ShapeDtypeStruct(queries.shape, jnp.bfloat16),
        in_specs=[smem, smem, hbm, hbm, hbm, vmem, vmem],
        out_specs=hbm,
        scratch_shapes=[
            whole(*queries.shape), whole(*features.shape), whole(*kv_weight.shape),
            whole(*queries.shape), whole(total, 2 * HD),
            whole(samples, tokens, width), whole(total, width),
            buffers(*wide), buffers(*half), buffers(*half), buffers(*wide), buffers(*wide),
            buffers(3, *wide), buffers(3, *wide),
            buffers(*wide), buffers(2, *wide), buffers(*wide), buffers(2, *wide),
            buffers(*wide), buffers(2, *wide), buffers(*wide), buffers(2, *wide),
            buffers(*half), buffers(*half),
            pltpu.SemaphoreType.DMA((PIECES * COPIES,)),
            pltpu.SemaphoreType.DMA((PIECES * COPIES,)),
            pltpu.SemaphoreType.DMA((samples,)),
            pltpu.SemaphoreType.DMA((samples,)),
            pltpu.SemaphoreType.DMA((samples + 2,)),
            pltpu.SemaphoreType.DMA((samples,)),
        ],
        compiler_params=pltpu.CompilerParams(
            collective_id=0, has_side_effects=True, vmem_limit_bytes=60 * 1024 * 1024
        ),
        name="exchange",
    )(
        owner, counts, queries, features, kv_weight, q_gain.reshape(1, HD), k_gain.reshape(1, HD)
    )


def solution(mesh):
    torus = Mesh(mesh.devices.reshape(4, 8, 2, 8, 2), (*DP, *TENSOR))
    in_specs = (P(DP, TENSOR), P(DP, None, TENSOR), P(TENSOR, None), P(), P(), P(), P())
    return jax.shard_map(
        shards, mesh=torus, in_specs=in_specs, out_specs=P(DP, TENSOR), check_vma=False
    )
```

```python
import math

import jax
import jax.numpy as jnp
from jax import lax
from jax.experimental import pallas as pl
from jax.experimental.pallas import tpu as pltpu
from jax.sharding import Mesh
from jax.sharding import PartitionSpec as P

HD = 128
PATCH = 24
PIECES = 8
COPIES = 18
OFFSETS = (0.0, 7.0, 8.0, 9.0, 9.5, 11.0, 12.5, 14.5, 16.5)
QUERY_TIME = 6.9
DP = ("x_lo", "z", "core")
TENSOR = ("y", "x_hi")
MESH = pl.DeviceIdType.MESH


def wrap(value, size):
    return lax.rem(value + 2 * size, size)


def widen(value):
    return value.astype(jnp.float32)


def narrow(value):
    return value.astype(jnp.bfloat16)


def normalize(values_in, gain):
    scale = lax.rsqrt(jnp.mean(values_in * values_in, axis=-1, keepdims=True) + 1e-05)
    return values_in * scale * gain


def body(
    owner_ref, counts_ref, query_hbm, feat_hbm, weight_hbm, q_gain_ref, k_gain_ref, out_hbm,
    query, feat, weight, result, both,
    partner, chosen, first, left0, right0, left1, right1, left, right,
    summed, cross, ready, near, turned, far, spun, side, twin_k, twin_v,
    send_sem, recv_sem, core_send, core_recv, load_sem, store_sem,
):
    x_lo, z, core = lax.axis_index("x_lo"), lax.axis_index("z"), lax.axis_index("core")
    y, x_hi = lax.axis_index("y"), lax.axis_index("x_hi")
    x = x_hi * 4 + x_lo
    samples, tokens = feat_hbm.shape[:2]
    rows = samples * tokens // PIECES
    per_sample = PIECES // samples
    text_len = query_hbm.shape[0] // samples
    heads = query_hbm.shape[1] // HD

    loads = []

    def load(source, target):
        copy = pltpu.make_async_copy(source, target, load_sem.at[len(loads)])
        copy.start()
        loads.append(copy)
        return copy

    feat_loads = [load(feat_hbm.at[j], feat.at[j]) for j in range(samples)]
    weight_load = load(weight_hbm, weight)
    query_load = load(query_hbm, query)

    def at_x(by):
        there = wrap(x + by, 8)
        return {"x_lo": lax.rem(there, 4), "x_hi": there // 4}

    def at_y(by):
        return {"y": wrap(y + by, 8)}

    def at_z(by):
        return {"z": wrap(z + by, 8)}

    other_core = {"core": 1 - core}

    barrier = pltpu.get_barrier_semaphore()
    peers = [at_y(-1), at_y(1), at_x(-2), at_x(2), at_x(-1), at_x(1)]
    peers += [at_z(-1), at_z(1), at_z(-3), at_z(3), other_core]
    for peer in peers:
        pl.semaphore_signal(barrier, inc=1, device_id=peer, device_id_type=MESH)
    pl.semaphore_wait(barrier, len(peers))

    core_copies = []
    for j in range(samples):
        copy = pltpu.make_async_remote_copy(
            src_ref=feat_hbm.at[j], dst_ref=partner.at[j],
            send_sem=core_send.at[j], recv_sem=core_recv.at[j],
            device_id=other_core, device_id_type=MESH,
        )
        copy.start()
        core_copies.append(copy)

    place = z * 2 + core
    plan, valid = [], []
    for j in range(samples):
        shift = owner_ref[j] // samples
        swap = lax.rem(shift, 2)
        low = lax.rem(shift, 16)
        borrow = jnp.where(place < low, 1, 0)
        along_z = lax.rem(lax.rem(shift // 2, 8) + swap * (1 - core), 8)
        along_x = lax.rem(shift // 16 + borrow + 2, 4)
        plan.append((swap, along_z, along_x))
        source = lax.rem(x_lo * 16 + place - shift + 64, 64)
        valid.append(counts_ref[source * samples + j] * PATCH)

    copies = {}

    def send(piece, number, source, target, device):
        copy = pltpu.make_async_remote_copy(
            src_ref=source, dst_ref=target,
            send_sem=send_sem.at[piece * COPIES + number],
            recv_sem=recv_sem.at[piece * COPIES + number],
            device_id=device, device_id_type=MESH,
        )
        copy.start()
        copies[piece, number] = copy

    def arrive(piece, *numbers):
        for number in numbers:
            copies[piece, number].wait_recv()

    def partial(piece, by):
        head = wrap(y + by, 8)
        columns = pl.ds(pl.multiple_of(head * 2 * HD, 2 * HD), 2 * HD)
        return jnp.dot(
            chosen[pl.ds(piece * rows, rows), :], weight[:, columns],
            preferred_element_type=jnp.float32,
        )

    def start_piece(p):
        j = p // per_sample
        if p % per_sample == 0:
            feat_loads[j].wait()
            if j == 0:
                weight_load.wait()
            core_copies[j].wait_recv()
            swapped = jnp.full((tokens, 1), plan[j][0], jnp.int32) == 1
            chosen[pl.ds(j * tokens, tokens), :] = jnp.where(swapped, partner[j], feat[j])
        first[p] = narrow(partial(p, 4))
        send(p, 0, first.at[p, :, pl.ds(0, HD)], left0.at[p], at_y(-1))
        send(p, 1, first.at[p, :, pl.ds(HD, HD)], right0.at[p], at_y(1))

    def second(p):
        to_left, to_right = partial(p, -3), partial(p, 3)
        arrive(p, 0, 1)
        left1[p, :, pl.ds(0, HD)] = narrow(to_left[:, :HD] + widen(left0[p]))
        left1[p, :, pl.ds(HD, HD)] = narrow(to_left[:, HD:])
        send(p, 2, left1.at[p], left.at[p, 0], at_y(-1))
        right1[p, :, pl.ds(0, HD)] = narrow(to_right[:, :HD])
        right1[p, :, pl.ds(HD, HD)] = narrow(to_right[:, HD:] + widen(right0[p]))
        send(p, 3, right1.at[p], right.at[p, 0], at_y(1))

    def later(p, step):
        to_left, to_right = partial(p, step - 3), partial(p, 3 - step)
        arrive(p, 2 * step, 2 * step + 1)
        left[p, step - 1] = narrow(to_left + widen(left[p, step - 1]))
        send(p, 2 * step + 2, left.at[p, step - 1], left.at[p, step], at_y(-1))
        right[p, step - 1] = narrow(to_right + widen(right[p, step - 1]))
        send(p, 2 * step + 3, right.at[p, step - 1], right.at[p, step], at_y(1))

    def own(p):
        mine = partial(p, 0)
        arrive(p, 6, 7)
        summed[p] = narrow(mine + widen(left[p, 2]) + widen(right[p, 2]))
        send(p, 8, summed.at[p], cross.at[p, 0], at_x(2))
        send(p, 9, summed.at[p], cross.at[p, 1], at_x(-2))

    def normed(p):
        arrive(p, 8, 9)
        total = widen(cross[p, 0]) + widen(cross[p, 1])
        ready[p, :, pl.ds(0, HD)] = narrow(normalize(total[:, :HD], k_gain_ref[...]))
        ready[p, :, pl.ds(HD, HD)] = narrow(total[:, HD:])
        send(p, 10, ready.at[p], near.at[p, 0], at_z(1))
        send(p, 11, ready.at[p], near.at[p, 1], at_z(-1))

    def pick(index, options):
        mask = jnp.full((rows, 1), index, jnp.int32)
        chosen_one = options[0]
        for number in range(1, len(options)):
            chosen_one = jnp.where(mask == number, options[number], chosen_one)
        return chosen_one

    def turn_near(p):
        arrive(p, 10, 11)
        s = plan[p // per_sample][1]
        plus = (s == 1) | (s == 4) | (s == 6)
        minus = (s == 2) | (s == 7)
        index = jnp.where(plus, 1, jnp.where(minus, 2, 0))
        turned[p] = pick(index, [ready[p], near[p, 0], near[p, 1]])
        send(p, 12, turned.at[p], far.at[p, 0], at_z(3))
        send(p, 13, turned.at[p], far.at[p, 1], at_z(-3))

    def turn_far(p):
        arrive(p, 12, 13)
        s = plan[p // per_sample][1]
        plus = (s == 2) | (s == 3) | (s == 4)
        minus = (s == 5) | (s == 6)
        index = jnp.where(plus, 1, jnp.where(minus, 2, 0))
        spun[p] = pick(index, [turned[p], far[p, 0], far[p, 1]])
        send(p, 14, spun.at[p], side.at[p, 0], at_x(1))
        send(p, 15, spun.at[p], side.at[p, 1], at_x(-1))
        send(p, 16, spun.at[p, :, pl.ds(0, HD)], twin_k.at[p], at_x(2))
        send(p, 17, spun.at[p, :, pl.ds(HD, HD)], twin_v.at[p], at_x(-2))

    def finish(p):
        arrive(p, 14, 15, 16, 17)
        u = plan[p // per_sample][2]
        for half, twin in enumerate((twin_k, twin_v)):
            part = pl.ds(half * HD, HD)
            both[pl.ds(p * rows, rows), part] = pick(
                u, [spun[p, :, part], side[p, 0, :, part], twin[p], side[p, 1, :, part]]
            )

    def prepare_queries():
        query_load.wait()
        for a in range(heads):
            part = pl.ds(a * HD, HD)
            normed_query = normalize(widen(query[:, part]), q_gain_ref[...])
            query[:, part] = narrow(normed_query / math.sqrt(HD))

    stores = []

    def attend(j):
        held = pl.ds(j * tokens, tokens)
        text = pl.ds(j * text_len, text_len)
        keys, values = both[held, pl.ds(0, HD)], both[held, pl.ds(HD, HD)]
        column = lax.broadcasted_iota(jnp.int32, (text_len, tokens), 1)
        for a in range(heads):
            part = pl.ds(a * HD, HD)
            scores = lax.dot_general(
                query[text, part], keys, (((1,), (1,)), ((), ())),
                preferred_element_type=jnp.float32,
            )
            exponent = jnp.where(column < valid[j], jnp.exp(scores), 0.0)
            weights = narrow(exponent / jnp.sum(exponent, axis=-1, keepdims=True))
            context = jnp.dot(weights, values, preferred_element_type=jnp.float32)
            result[text, part] = narrow(context)
        copy = pltpu.make_async_copy(result.at[text], out_hbm.at[text], store_sem.at[j])
        copy.start()
        stores.append(copy)

    stages = [start_piece, second, lambda p: later(p, 1), lambda p: later(p, 2), own, normed]
    stages += [turn_near, turn_far, finish]
    tasks = [(QUERY_TIME, 1, prepare_queries, ())]
    for number, (stage, offset) in enumerate(zip(stages, OFFSETS)):
        tasks += [(p + offset, -number, stage, (p,)) for p in range(PIECES)]
    for j in range(samples):
        tasks.append(((j + 1) * per_sample - 1 + OFFSETS[-1], 1, attend, (j,)))
    for _, _, task, given in sorted(tasks, key=lambda task: task[:2]):
        task(*given)
    for copy in core_copies + list(copies.values()):
        copy.wait_send()
    for copy in stores:
        copy.wait()


def shards(queries, features, kv_weight, q_gain, k_gain, counts, owner):
    samples, tokens, width = features.shape
    total = samples * tokens
    rows = total // PIECES
    wide, half = (rows, 2 * HD), (rows, HD)

    def whole(*shape):
        return pltpu.VMEM(shape, jnp.bfloat16)

    def buffers(*shape):
        return whole(PIECES, *shape)

    smem = pl.BlockSpec(memory_space=pltpu.SMEM)
    vmem = pl.BlockSpec(memory_space=pltpu.VMEM)
    hbm = pl.BlockSpec(memory_space=pltpu.HBM)
    return pl.pallas_call(
        body,
        out_shape=jax.ShapeDtypeStruct(queries.shape, jnp.bfloat16),
        in_specs=[smem, smem, hbm, hbm, hbm, vmem, vmem],
        out_specs=hbm,
        scratch_shapes=[
            whole(*queries.shape), whole(*features.shape), whole(*kv_weight.shape),
            whole(*queries.shape), whole(total, 2 * HD),
            whole(samples, tokens, width), whole(total, width),
            buffers(*wide), buffers(*half), buffers(*half), buffers(*wide), buffers(*wide),
            buffers(3, *wide), buffers(3, *wide),
            buffers(*wide), buffers(2, *wide), buffers(*wide), buffers(2, *wide),
            buffers(*wide), buffers(2, *wide), buffers(*wide), buffers(2, *wide),
            buffers(*half), buffers(*half),
            pltpu.SemaphoreType.DMA((PIECES * COPIES,)),
            pltpu.SemaphoreType.DMA((PIECES * COPIES,)),
            pltpu.SemaphoreType.DMA((samples,)),
            pltpu.SemaphoreType.DMA((samples,)),
            pltpu.SemaphoreType.DMA((samples + 2,)),
            pltpu.SemaphoreType.DMA((samples,)),
        ],
        compiler_params=pltpu.CompilerParams(
            collective_id=0, has_side_effects=True, vmem_limit_bytes=60 * 1024 * 1024
        ),
        name="exchange",
    )(
        owner, counts, queries, features, kv_weight, q_gain.reshape(1, HD), k_gain.reshape(1, HD)
    )


def solution(mesh):
    torus = Mesh(mesh.devices.reshape(4, 8, 2, 8, 2), (*DP, *TENSOR))
    in_specs = (P(DP, TENSOR), P(DP, None, TENSOR), P(TENSOR, None), P(), P(), P(), P())
    return jax.shard_map(
        shards, mesh=torus, in_specs=in_specs, out_specs=P(DP, TENSOR), check_vma=False
    )
```
